256 devices in a mesh: date: 16 (over z, core), pix: 16 (over y, x).
Axes of the slice: x: 4, y: 4, z: 8, core: 2. Of those that a mesh axis runs over, the one named last changes fastest.
Arguments:
- bin_index: int32 [256, 1048576], P('date', 'pix'), may hold values from 0 to 511
- clear_mask: bfloat16 [256, 1048576], P('date', 'pix'), may hold values from 0 to 1, as said below
Outputs:
- anomaly: float32 [3, 8192], P(None, 'pix')
- tile_levels: float32 [3], replicated
The draws below stay inside these ranges and needn't reach their ends.
Inputs may be any that keep to these rules, and one draw needn't show every extreme that they name: `clear_mask`: 0 for a cloudy observation, else a positive weight.
All inputs are finite; a program needn't handle non-finite values.
Results may differ from the reference program's by a relative error of at most 0.0003.
Values sent between devices are 32-bit elements; how exact they have to be, the bound alone decides.
A program may use at most 64 MiB of HBM per device.

```python
import jax
import jax.numpy as jnp
from jax import lax

BINS = 512
BLOCK = 128
DATES = 256
BLOCKS = 8192
PIXELS = 1048576


def draw_bin_index(key, part):
    keys = jax.random.split(jax.random.fold_in(key, 11), 8)
    dates = jnp.arange(DATES, dtype=jnp.int32)
    pixels = jnp.arange(PIXELS, dtype=jnp.int32)
    mode_bins = jax.random.randint(keys[0], (BLOCKS, 4), 8, BINS - 8)
    spike_offsets = jax.random.randint(keys[1], (BLOCKS, 4, 4), -7, 8)
    boundaries = jnp.sort(jax.random.randint(keys[2], (BLOCKS, 3), 0, 65), axis=1)
    owner = pixels // BLOCK
    ticket = jax.random.randint(keys[3], (PIXELS,), 0, 64)
    first_mode = jnp.sum((ticket[:, None] >= boundaries[owner]).astype(jnp.int32), axis=1)
    turning = jax.random.randint(keys[4], (PIXELS,), 0, 4)
    season_section = 3 * dates // DATES
    chosen = (first_mode[None] + season_section[:, None] * turning[None]) % 4
    picked = jax.random.randint(keys[5], (DATES, PIXELS), 0, 4)
    mode_slot = owner[None] * 4 + chosen
    located = mode_bins.reshape(-1)[mode_slot] + spike_offsets.reshape(-1)[mode_slot * 4 + picked]
    moded = jnp.clip(located, 0, BINS - 1)
    stray_flag = jax.random.randint(keys[6], (DATES, PIXELS), 0, 3) == 0
    stray_bins = jax.random.randint(keys[7], (DATES, PIXELS), 0, BINS)
    return jnp.where(stray_flag, stray_bins, moded).astype(jnp.int32)


def draw_clear_mask(key, part):
    keys = jax.random.split(jax.random.fold_in(key, 23), 3)
    keeping = jax.random.randint(keys[0], (DATES, BLOCKS, 1), 1, 20)
    rolled = jax.random.randint(keys[1], (DATES, BLOCKS, BLOCK), 0, 20)
    weights = jax.random.uniform(keys[2], (DATES, BLOCKS, BLOCK), jnp.float32, 0.3, 1.0)
    values = jnp.where(rolled < keeping, weights, jnp.zeros((), jnp.float32))
    return values.reshape(DATES, PIXELS).astype(jnp.bfloat16)


def setup_inputs(seed: int = 0) -> dict:
    splits = jax.random.split(jax.random.key(seed), 3)
    return {
        "bin_index": draw_bin_index(jax.random.fold_in(splits[2], 71), 0),
        "clear_mask": draw_clear_mask(jax.random.fold_in(splits[2], 71), 0),
    }


QUANTILES = (0.1, 0.5, 0.9)
LOW_EDGE = -1.0


def percentiles(counts, before, totals):
    target = jnp.stack([quantile * totals + 0.25 for quantile in QUANTILES])
    passed = jnp.clip((target[:, :, None] - before[None]) / jnp.maximum(counts, 1.0)[None], 0.0, 1.0)
    return LOW_EDGE + (2.0 / BINS) * jnp.sum(passed, axis=2)


def reference(bin_index, clear_mask):
    block_base = jnp.arange(PIXELS, dtype=jnp.int32) // BLOCK * BINS

    def add_frame(totals, frame_pair):
        frame_bins, frame_clear = frame_pair
        return totals.at[block_base + frame_bins].add(frame_clear.astype(jnp.float32)), None

    flat_counts, unused = lax.scan(add_frame, jnp.zeros((BLOCKS * BINS,), jnp.float32), (bin_index, clear_mask))
    counts = flat_counts.reshape(BLOCKS, BINS)
    tile_counts = jnp.sum(counts, axis=0)
    tile_before = jnp.cumsum(tile_counts) - tile_counts
    tile_levels = percentiles(tile_counts[None], tile_before[None], jnp.sum(tile_counts)[None])[:, 0]
    block_before = jnp.cumsum(counts, axis=1) - counts
    block_levels = percentiles(counts, block_before, jnp.sum(counts, axis=1))
    return block_levels - tile_levels[:, None], tile_levels
```

```python
import functools

import jax
import jax.numpy as jnp
from jax import lax
from jax.experimental import pallas as pl
from jax.experimental.pallas import tpu as pltpu
from jax.sharding import PartitionSpec as P

BINS = 512
BLOCK = 128
UPPER = 16
LOWER = 32
JOINED = 8
QUANTILES = (0.1, 0.5, 0.9)
LOW_EDGE = -1.0
MESH = pl.DeviceIdType.MESH
bf16 = jnp.bfloat16
f32 = jnp.float32
f8 = jnp.float8_e4m3fn


def iota(shape, dim):
    return lax.broadcasted_iota(jnp.int32, shape, dim)


def ones_where(mask):
    return jnp.where(mask, 1.0, 0.0).astype(bf16)


def pieces(x):
    first = x.astype(bf16)
    rest = x - first.astype(f32)
    second = rest.astype(bf16)
    third = (rest - second.astype(f32)).astype(bf16)
    return first, second, third


def count_group(idx_ref, w_ref, base, acc, mxu):
    upper_rows = (iota((UPPER, 128), 0) * LOWER).astype(jnp.int16)
    lower_rows = iota((LOWER, 128), 0).astype(jnp.int16)
    lefts, rights = [], []
    frames = idx_ref.shape[0]
    for j in range(JOINED):
        lanes = pl.ds(pl.multiple_of(base + 128 * j, 128), 128)
        bins = idx_ref[:, lanes].astype(jnp.int16)
        weight = w_ref[:, lanes]
        upper = bins & jnp.int16((UPPER - 1) * LOWER)
        lower = bins & jnp.int16(LOWER - 1)
        left, right = [], []
        for f in range(frames):
            row = slice(f, f + 1)
            is_upper = jnp.broadcast_to(upper[row], (UPPER, 128)) == upper_rows
            is_lower = jnp.broadcast_to(lower[row], (LOWER, 128)) == lower_rows
            left.append(jnp.where(is_upper, jnp.broadcast_to(weight[row], (UPPER, 128)), jnp.zeros((), bf16)))
            right.append(jnp.where(is_lower, jnp.ones((), f8), jnp.zeros((), f8)))
        lefts.append(left)
        rights.append(right)
    for k in range(frames // 2):
        pair = (2 * k, 2 * k + 1)
        left = jnp.concatenate([jnp.concatenate([x[f] for f in pair], axis=1) for x in lefts], axis=0)
        right = jnp.concatenate([jnp.concatenate([x[f] for f in pair], axis=1) for x in rights], axis=0)
        pltpu.matmul_push_rhs(right, staging_register=k % 2, mxu_index=mxu, transpose=True)
        pltpu.matmul_acc_lhs(acc, left, load_staged_rhs=k % 2)
    joint = pltpu.matmul_pop(acc)
    lane = iota((UPPER, 128), 1)
    halves = []
    for half in range(2):
        own = None
        for q in range(4):
            j = 4 * half + q
            part = joint[j * UPPER : (j + 1) * UPPER, half * 128 : (half + 1) * 128]
            own = part if own is None else jnp.where(lane >= q * LOWER, part, own)
        halves.append(own)
    return jnp.concatenate(halves, axis=1)


def triple_matmul(acc, x, register):
    for n, piece in enumerate(pieces(x)):
        pltpu.matmul_acc_lhs(acc, piece, load_staged_rhs=register if n == 0 else None)


def block_levels(counts, acc_prefix, acc_rows, acc_below, acc_sums):
    flat = counts.reshape(64, 256)
    r, c = iota((256, 256), 0), iota((256, 256), 1)
    same = (r // LOWER) == (c // LOWER)
    pltpu.matmul_push_rhs(ones_where(same & (r % LOWER < c % LOWER)), staging_register=0, mxu_index=0)
    pltpu.matmul_push_rhs(ones_where(same), staging_register=0, mxu_index=1)
    triple_matmul(acc_prefix, flat, 0)
    triple_matmul(acc_rows, flat, 0)
    row_sums = pltpu.matmul_pop(acc_rows)
    stacked = jnp.concatenate([*pieces(row_sums), jnp.zeros((64, 256), bf16)], axis=0)
    pltpu.matmul_push_rhs(stacked, staging_register=0, mxu_index=0)
    i, k = iota((128, 256), 0), iota((128, 256), 1)
    chosen = ((i % 64) // UPPER == (k % 64) // UPPER) & (k < 192) & ((k % UPPER < i % UPPER) | (i >= 64))
    pltpu.matmul_acc_lhs(acc_below, ones_where(chosen), load_staged_rhs=0)
    within = pltpu.matmul_pop(acc_prefix)
    below = pltpu.matmul_pop(acc_below)
    before = within + below[:64]
    total = below[64:]
    floor = jnp.maximum(flat, 1.0)
    passed = [jnp.clip((q * total + 0.25 - before) / floor, 0.0, 1.0) for q in QUANTILES]
    for g in range(4):
        pltpu.matmul_push_rhs(
            ones_where((c % LOWER) == JOINED * g + r // LOWER), staging_register=0, mxu_index=1
        )
        rows = jnp.concatenate([p[g * UPPER : (g + 1) * UPPER] for p in passed], axis=0)
        triple_matmul(acc_sums, rows, 0)
    sums = pltpu.matmul_pop(acc_sums)[:, :128]
    row = iota((8, 128), 0)
    out = jnp.zeros((8, 128), f32)
    for q in range(3):
        value = jnp.sum(sums[q * UPPER : (q + 1) * UPPER], axis=0, keepdims=True)
        out = jnp.where(row == q, LOW_EDGE + 2.0 / BINS * value, out)
    return out


def push_tile_tables(register):
    r, c = iota((256, 256), 0), iota((256, 256), 1)
    same = (r % 128) // 64 == (c % 128) // 64
    counts = same & (r % LOWER == c % LOWER) & (c < 128)
    prefix = same & (r % LOWER < c % LOWER) & (c >= 128)
    pltpu.matmul_push_rhs(ones_where(counts | prefix), staging_register=register, mxu_index=0)
    pltpu.matmul_push_rhs(ones_where(same | (c >= 128)), staging_register=register, mxu_index=1)


def tile_of(total, acc_a, acc_b, register):
    p1, p2, p3 = pieces(total)
    zero = jnp.zeros((8, 128), f32)
    left = jnp.concatenate(
        [
            jnp.concatenate([p1.astype(f32), p3.astype(f32)], axis=0),
            jnp.concatenate([p2.astype(f32), zero], axis=0),
        ],
        axis=1,
    ).astype(bf16)
    pltpu.matmul_acc_lhs(acc_a, left, load_staged_rhs=register)
    pltpu.matmul_acc_lhs(acc_b, left, load_staged_rhs=register)
    a = pltpu.matmul_pop(acc_a)
    b = pltpu.matmul_pop(acc_b)
    a = a[:8] + a[8:]
    b = b[:8] + b[8:]
    counts, within = a[:, :128], a[:, 128:]
    same_rows, all_rows = b[:, :128], b[:, 128:]
    row, lane = iota((8, 128), 0), iota((8, 128), 1)
    below = jnp.where(row >= 1, pltpu.roll(same_rows, 1, 0), 0.0)
    for shift in (1, 2, 4):
        below = below + jnp.where(row >= shift, pltpu.roll(below, shift, 0), 0.0)
        same_rows = same_rows + pltpu.roll(same_rows, shift, 0)
        all_rows = all_rows + pltpu.roll(all_rows, shift, 0)
    before = within + below + jnp.where(lane >= 64, all_rows - same_rows, 0.0)
    floor = jnp.maximum(counts, 1.0)
    levels = []
    for q in QUANTILES:
        passed = jnp.clip((q * all_rows + 0.25 - before) / floor, 0.0, 1.0)
        both = jnp.sum(jnp.sum(passed, axis=0, keepdims=True), axis=1, keepdims=True)
        levels.append(LOW_EDGE + 2.0 / BINS * (0.5 * both))
    return levels


def kernel(
    dates,
    pixs,
    idx_hbm,
    w_hbm,
    anomaly_ref,
    tile_ref,
    idx_v,
    w_v,
    raw,
    part_out,
    part_in,
    own,
    ici_in,
    tile_acc,
    pix_in,
    date_in,
    level_in,
    in_sem,
    core_send,
    core_recv,
    ici_send,
    ici_recv,
    pix_send,
    pix_recv,
    date_send,
    date_recv,
    level_send,
    level_recv,
):
    d = lax.axis_index("date")
    p = lax.axis_index("pix")
    z = lax.div(d, 2)
    core = lax.rem(d, 2)
    rings = dates // 2
    owner_lanes = idx_v.shape[1] // dates
    chunk = 2 * owner_lanes
    half = rings // 2

    def offset_of(s):
        odd = lax.rem(s, 2)
        return half + (1 - odd) * lax.div(s, 2) - odd * lax.div(s + 1, 2)

    def ring_at(s):
        return lax.rem(z + offset_of(s), rings)

    def load(s):
        lanes = pl.ds(pl.multiple_of(ring_at(s) * chunk, 128), chunk)
        return (
            pltpu.make_async_copy(idx_hbm.at[:, lanes], idx_v.at[:, lanes], in_sem.at[0, s]),
            pltpu.make_async_copy(w_hbm.at[:, lanes], w_v.at[:, lanes], in_sem.at[1, s]),
        )

    for s in range(rings):
        for copy in load(s):
            copy.start()

    barrier = pltpu.get_barrier_semaphore()
    for k in range(1, dates):
        pl.semaphore_signal(barrier, inc=1, device_id={"date": lax.rem(d + k, dates)}, device_id_type=MESH)
    for k in range(1, pixs):
        pl.semaphore_signal(barrier, inc=1, device_id={"pix": lax.rem(p + k, pixs)}, device_id_type=MESH)

    def to_core(s):
        return pltpu.make_async_remote_copy(
            src_ref=part_out.at[s],
            dst_ref=part_in.at[s],
            send_sem=core_send.at[s],
            recv_sem=core_recv.at[s],
            device_id={"date": d + 1 - 2 * core},
            device_id_type=MESH,
        )

    def to_ring(s):
        off = offset_of(s)
        return pltpu.make_async_remote_copy(
            src_ref=own.at[s],
            dst_ref=ici_in.at[off],
            send_sem=ici_send.at[s],
            recv_sem=ici_recv.at[off],
            device_id={"date": 2 * lax.rem(z + off, rings) + core},
            device_id_type=MESH,
        )

    def to_all(buffer, axis, me, size, k, send, recv):
        return pltpu.make_async_remote_copy(
            src_ref=buffer.at[me],
            dst_ref=buffer.at[me],
            send_sem=send.at[k],
            recv_sem=recv.at[me],
            device_id={axis: lax.rem(me + k, size)},
            device_id_type=MESH,
        )

    def from_all(buffer, axis, me, size, k, send, recv):
        source = lax.rem(me + k, size)
        return pltpu.make_async_remote_copy(
            src_ref=buffer.at[source],
            dst_ref=buffer.at[source],
            send_sem=send.at[k],
            recv_sem=recv.at[source],
            device_id={axis: source},
            device_id_type=MESH,
        )

    to_pix = (pix_in, "pix", p, pixs)
    to_date = (date_in, "date", d, dates)
    to_level = (level_in, "date", d, dates)

    def body(acc_a, acc_b, acc_c, acc_d, acc_prefix, acc_rows, acc_sums, acc_ta, acc_tb):
        tile_acc[...] = jnp.zeros_like(tile_acc)

        def step(s, carry):
            for copy in load(s):
                copy.wait()
            ring = ring_at(s)
            sums = None
            for m in range(8):
                side = 1 - core if m < 4 else core
                base = (2 * ring + side) * owner_lanes + (m % 4) * (JOINED * BLOCK)
                counts = count_group(idx_v, w_v, base, (acc_a, acc_b, acc_c, acc_d)[m % 4], m % 2)
                if m < 4:
                    part_out[s, m] = counts
                else:
                    raw[s, m - 4] = counts
                sums = counts if sums is None else sums + counts
            tile_acc[...] += sums

            @pl.when(s == 0)
            def _():
                pl.semaphore_wait(barrier, dates + pixs - 2)

            @pl.when(s >= 1)
            def _():
                to_core(s - 1).wait_recv()
                own[s - 1] = raw[s - 1] + part_in[s - 1]

            to_core(s).start()

            @pl.when(s >= 1)
            def _():
                to_ring(s - 1).start()

            return carry

        lax.fori_loop(0, rings, step, 0)

        lane = iota((8, 128), 1)
        folded = tile_acc[:, :128] + tile_acc[:, 128:]
        folded = folded + pltpu.roll(folded, 64, 1)
        pix_in[p] = jnp.where(lane < 64, folded[:8], folded[8:])
        for k in range(1, pixs):
            to_all(*to_pix, k, pix_send, pix_recv).start()

        to_core(rings - 1).wait_recv()
        mine = raw[rings - 1] + part_in[rings - 1]

        for k in range(1, pixs):
            from_all(*to_pix, k, pix_send, pix_recv).wait_recv()
        total = pix_in[0]
        for k in range(1, pixs):
            total = total + pix_in[k]
        date_in[d] = total
        for k in range(1, dates):
            to_all(*to_date, k, date_send, date_recv).start()

        for s in range(rings - 1):
            to_ring(s).wait_recv()
        for off in range(1, rings):
            mine = mine + ici_in[off]
        level_in[d] = block_levels(mine, acc_prefix, acc_rows, acc_a, acc_sums)
        for k in range(1, dates):
            to_all(*to_level, k, level_send, level_recv).start()

        push_tile_tables(1)
        for k in range(1, dates):
            from_all(*to_date, k, date_send, date_recv).wait_recv()
        total = date_in[0]
        for k in range(1, dates):
            total = total + date_in[k]
        levels = tile_of(total, acc_ta, acc_tb, 1)
        row = iota((8, 128), 0)
        by_lane = jnp.where(lane == 0, levels[0], jnp.where(lane == 1, levels[1], levels[2]))
        by_row = jnp.where(row == 0, levels[0], jnp.where(row == 1, levels[1], levels[2]))
        tile_ref[...] = by_lane[:1]

        for k in range(1, dates):
            from_all(*to_level, k, level_send, level_recv).wait_recv()
        for v in range(4):
            wide = level_in[4 * v]
            for i in range(1, 4):
                wide = jnp.where(lane >= 32 * i, level_in[4 * v + i], wide)
            anomaly_ref[:, v * 128 : (v + 1) * 128] = (wide - by_row)[:3]

        for s in range(rings):
            to_core(s).wait_send()
        for s in range(rings - 1):
            to_ring(s).wait_send()
        for k in range(1, pixs):
            to_all(*to_pix, k, pix_send, pix_recv).wait_send()
        for k in range(1, dates):
            to_all(*to_date, k, date_send, date_recv).wait_send()
            to_all(*to_level, k, level_send, level_recv).wait_send()

    pl.run_scoped(
        body,
        pltpu.ACC(0)((128, 256), f32),
        pltpu.ACC(1)((128, 256), f32),
        pltpu.ACC(0)((128, 256), f32),
        pltpu.ACC(1)((128, 256), f32),
        pltpu.ACC(0)((64, 256), f32),
        pltpu.ACC(1)((64, 256), f32),
        pltpu.ACC(1)((48, 256), f32),
        pltpu.ACC(0)((16, 256), f32),
        pltpu.ACC(1)((16, 256), f32),
    )


def solution(mesh):
    dates, pixs = mesh.shape["date"], mesh.shape["pix"]
    rings = dates // 2

    def body(bin_index, clear_mask):
        frames, pixels = bin_index.shape
        blocks = pixels // BLOCK
        groups = blocks // dates // JOINED
        quarter = (rings, groups, UPPER, JOINED * LOWER)
        dma = pltpu.SemaphoreType.DMA
        anomaly, tile = pl.pallas_call(
            functools.partial(kernel, dates, pixs),
            out_shape=(
                jax.ShapeDtypeStruct((3, blocks), f32),
                jax.ShapeDtypeStruct((1, 128), f32),
            ),
            in_specs=[pl.BlockSpec(memory_space=pltpu.HBM)] * 2,
            out_specs=(pl.BlockSpec(memory_space=pltpu.VMEM),) * 2,
            scratch_shapes=[
                pltpu.VMEM((frames, pixels), jnp.int32),
                pltpu.VMEM((frames, pixels), bf16),
                *[pltpu.VMEM(quarter, f32) for _ in range(5)],
                pltpu.VMEM((UPPER, JOINED * LOWER), f32),
                pltpu.VMEM((pixs, 8, 128), f32),
                pltpu.VMEM((dates, 8, 128), f32),
                pltpu.VMEM((dates, 8, 128), f32),
                dma((2, rings)),
                dma((rings,)),
                dma((rings,)),
                dma((rings,)),
                dma((rings,)),
                dma((pixs,)),
                dma((pixs,)),
                dma((dates,)),
                dma((dates,)),
                dma((dates,)),
                dma((dates,)),
            ],
            compiler_params=pltpu.CompilerParams(collective_id=0, has_side_effects=True),
        )(bin_index, clear_mask)
        return anomaly, tile[0, :3]

    return jax.shard_map(
        body,
        mesh=mesh,
        in_specs=(P("date", "pix"), P("date", "pix")),
        out_specs=(P(None, "pix"), P()),
        check_vma=False,
    )
```

```python
import functools

import jax
import jax.numpy as jnp
from jax import lax
from jax.experimental import pallas as pl
from jax.experimental.pallas import tpu as pltpu
from jax.sharding import PartitionSpec as P

BINS = 512
BLOCK = 128
UPPER = 16
LOWER = 32
JOINED = 8
QUANTILES = (0.1, 0.5, 0.9)
LOW_EDGE = -1.0
AHEAD = (4, 2, 2, 3, 3, 1, 1, 0)
HALF_AHEAD = (0, 0, 1, 0, 1, 0, 1, 0)
HALF_BEHIND = (1, 0, 1, 0, 1, 0, 1, 1)
FIRST_RELAYED = 3
MESH = pl.DeviceIdType.MESH
bf16 = jnp.bfloat16
f32 = jnp.float32
f8 = jnp.float8_e4m3fn


def iota(shape, dim):
    return lax.broadcasted_iota(jnp.int32, shape, dim)


def ones_where(mask):
    return jnp.where(mask, 1.0, 0.0).astype(bf16)


def pieces(x):
    first = x.astype(bf16)
    rest = x - first.astype(f32)
    second = rest.astype(bf16)
    third = (rest - second.astype(f32)).astype(bf16)
    return first, second, third


def feed_group(idx_ref, w_ref, base, acc, mxu):
    upper_rows = (iota((UPPER, 128), 0) * LOWER).astype(jnp.int16)
    lower_rows = iota((LOWER, 128), 0).astype(jnp.int16)
    lefts, rights = [], []
    frames = idx_ref.shape[0]
    for j in range(JOINED):
        lanes = pl.ds(pl.multiple_of(base + 128 * j, 128), 128)
        bins = idx_ref[:, lanes].astype(jnp.int16)
        weight = w_ref[:, lanes]
        upper = bins & jnp.int16((UPPER - 1) * LOWER)
        lower = bins & jnp.int16(LOWER - 1)
        left, right = [], []
        for f in range(frames):
            row = slice(f, f + 1)
            is_upper = jnp.broadcast_to(upper[row], (UPPER, 128)) == upper_rows
            is_lower = jnp.broadcast_to(lower[row], (LOWER, 128)) == lower_rows
            left.append(jnp.where(is_upper, jnp.broadcast_to(weight[row], (UPPER, 128)), jnp.zeros((), bf16)))
            right.append(jnp.where(is_lower, jnp.ones((), f8), jnp.zeros((), f8)))
        lefts.append(left)
        rights.append(right)
    for k in range(frames // 2):
        pair = (2 * k, 2 * k + 1)
        left = jnp.concatenate([jnp.concatenate([x[f] for f in pair], axis=1) for x in lefts], axis=0)
        right = jnp.concatenate([jnp.concatenate([x[f] for f in pair], axis=1) for x in rights], axis=0)
        pltpu.matmul_push_rhs(right, staging_register=k % 2, mxu_index=mxu, transpose=True)
        pltpu.matmul_acc_lhs(acc, left, load_staged_rhs=k % 2)


def drain_group(acc):
    joint = pltpu.matmul_pop(acc)
    lane = iota((UPPER, 128), 1)
    halves = []
    for half in range(2):
        own = None
        for q in range(4):
            j = 4 * half + q
            part = joint[j * UPPER : (j + 1) * UPPER, half * 128 : (half + 1) * 128]
            own = part if own is None else jnp.where(lane >= q * LOWER, part, own)
        halves.append(own)
    return jnp.concatenate(halves, axis=1)


def triple_matmul(acc, x, register):
    for n, piece in enumerate(pieces(x)):
        pltpu.matmul_acc_lhs(acc, piece, load_staged_rhs=register if n == 0 else None)


def block_levels(counts, acc_prefix, acc_rows, acc_below, acc_sums):
    flat = counts.reshape(64, 256)
    r, c = iota((256, 256), 0), iota((256, 256), 1)
    same = (r // LOWER) == (c // LOWER)
    pltpu.matmul_push_rhs(ones_where(same & (r % LOWER < c % LOWER)), staging_register=0, mxu_index=0)
    pltpu.matmul_push_rhs(ones_where(same), staging_register=0, mxu_index=1)
    triple_matmul(acc_prefix, flat, 0)
    triple_matmul(acc_rows, flat, 0)
    row_sums = pltpu.matmul_pop(acc_rows)
    stacked = jnp.concatenate([*pieces(row_sums), jnp.zeros((64, 256), bf16)], axis=0)
    pltpu.matmul_push_rhs(stacked, staging_register=0, mxu_index=0)
    i, k = iota((128, 256), 0), iota((128, 256), 1)
    chosen = ((i % 64) // UPPER == (k % 64) // UPPER) & (k < 192) & ((k % UPPER < i % UPPER) | (i >= 64))
    pltpu.matmul_acc_lhs(acc_below, ones_where(chosen), load_staged_rhs=0)
    within = pltpu.matmul_pop(acc_prefix)
    below = pltpu.matmul_pop(acc_below)
    before = within + below[:64]
    total = below[64:]
    floor = jnp.maximum(flat, 1.0)
    passed = [jnp.clip((q * total + 0.25 - before) / floor, 0.0, 1.0) for q in QUANTILES]
    for g in range(4):
        pltpu.matmul_push_rhs(
            ones_where((c % LOWER) == JOINED * g + r // LOWER), staging_register=0, mxu_index=1
        )
        rows = jnp.concatenate([p[g * UPPER : (g + 1) * UPPER] for p in passed], axis=0)
        triple_matmul(acc_sums, rows, 0)
    sums = pltpu.matmul_pop(acc_sums)[:, :128]
    row = iota((8, 128), 0)
    out = jnp.zeros((8, 128), f32)
    for q in range(3):
        value = jnp.sum(sums[q * UPPER : (q + 1) * UPPER], axis=0, keepdims=True)
        out = jnp.where(row == q, LOW_EDGE + 2.0 / BINS * value, out)
    return out


def push_tile_tables(register):
    r, c = iota((256, 256), 0), iota((256, 256), 1)
    same = (r % 128) // 64 == (c % 128) // 64
    counts = same & (r % LOWER == c % LOWER) & (c < 128)
    prefix = same & (r % LOWER < c % LOWER) & (c >= 128)
    pltpu.matmul_push_rhs(ones_where(counts | prefix), staging_register=register, mxu_index=0)
    pltpu.matmul_push_rhs(ones_where(same | (c >= 128)), staging_register=register, mxu_index=1)


def tile_of(total, acc_a, acc_b, register):
    p1, p2, p3 = pieces(total)
    zero = jnp.zeros((8, 128), f32)
    left = jnp.concatenate(
        [
            jnp.concatenate([p1.astype(f32), p3.astype(f32)], axis=0),
            jnp.concatenate([p2.astype(f32), zero], axis=0),
        ],
        axis=1,
    ).astype(bf16)
    pltpu.matmul_acc_lhs(acc_a, left, load_staged_rhs=register)
    pltpu.matmul_acc_lhs(acc_b, left, load_staged_rhs=register)
    a = pltpu.matmul_pop(acc_a)
    b = pltpu.matmul_pop(acc_b)
    a = a[:8] + a[8:]
    b = b[:8] + b[8:]
    counts, within = a[:, :128], a[:, 128:]
    same_rows, all_rows = b[:, :128], b[:, 128:]
    row, lane = iota((8, 128), 0), iota((8, 128), 1)
    below = jnp.where(row >= 1, pltpu.roll(same_rows, 1, 0), 0.0)
    for shift in (1, 2, 4):
        below = below + jnp.where(row >= shift, pltpu.roll(below, shift, 0), 0.0)
        same_rows = same_rows + pltpu.roll(same_rows, shift, 0)
        all_rows = all_rows + pltpu.roll(all_rows, shift, 0)
    before = within + below + jnp.where(lane >= 64, all_rows - same_rows, 0.0)
    floor = jnp.maximum(counts, 1.0)
    levels = []
    for q in QUANTILES:
        passed = jnp.clip((q * all_rows + 0.25 - before) / floor, 0.0, 1.0)
        both = jnp.sum(jnp.sum(passed, axis=0, keepdims=True), axis=1, keepdims=True)
        levels.append(LOW_EDGE + 2.0 / BINS * (0.5 * both))
    return levels


def kernel(
    dates,
    pixs,
    idx_hbm,
    w_hbm,
    anomaly_ref,
    tile_ref,
    idx_v,
    w_v,
    raw,
    part_out,
    part_in,
    own,
    ici_in,
    relay_in,
    tile_acc,
    pix_in,
    date_in,
    level_in,
    in_sem,
    core_send,
    core_recv,
    ici_send,
    ici_recv,
    relay_send,
    relay_recv,
    pix_send,
    pix_recv,
    date_send,
    date_recv,
    level_send,
    level_recv,
):
    d = lax.axis_index("date")
    p = lax.axis_index("pix")
    z = lax.div(d, 2)
    core = lax.rem(d, 2)
    rings = dates // 2
    owner_lanes = idx_v.shape[1] // dates
    chunk = 2 * owner_lanes

    def load(off):
        ring = lax.rem(z + off, rings)
        lanes = pl.ds(pl.multiple_of(ring * chunk, 128), chunk)
        return (
            pltpu.make_async_copy(idx_hbm.at[:, lanes], idx_v.at[:, lanes], in_sem.at[0, ring]),
            pltpu.make_async_copy(w_hbm.at[:, lanes], w_v.at[:, lanes], in_sem.at[1, ring]),
        )

    for off in (4, 2, 6, 3, 5, 1, 7, 0):
        for copy in load(off):
            copy.start()

    barrier = pltpu.get_barrier_semaphore()
    for k in range(1, dates):
        pl.semaphore_signal(barrier, inc=1, device_id={"date": lax.rem(d + k, dates)}, device_id_type=MESH)
    for k in range(1, pixs):
        pl.semaphore_signal(barrier, inc=1, device_id={"pix": lax.rem(p + k, pixs)}, device_id_type=MESH)

    def to_core(s):
        return pltpu.make_async_remote_copy(
            src_ref=part_out.at[s],
            dst_ref=part_in.at[s],
            send_sem=core_send.at[0],
            recv_sem=core_recv.at[s],
            device_id={"date": d + 1 - 2 * core},
            device_id_type=MESH,
        )

    def to_ring(s, off, side, half):
        groups = pl.ds(2 * half, 2)
        return pltpu.make_async_remote_copy(
            src_ref=own.at[s, pl.ds(2 * side, 2)],
            dst_ref=ici_in.at[off, groups],
            send_sem=ici_send.at[0],
            recv_sem=ici_recv.at[0],
            device_id={"date": 2 * lax.rem(z + off, rings) + core},
            device_id_type=MESH,
        )

    def all_rings():
        whole = own.at[pl.ds(0, rings - 2)]
        return pltpu.make_async_remote_copy(
            src_ref=whole,
            dst_ref=ici_in.at[pl.ds(0, rings - 2)],
            send_sem=ici_send.at[0],
            recv_sem=ici_recv.at[0],
            device_id={"date": d + 1 - 2 * core},
            device_id_type=MESH,
        )

    def all_cores():
        return pltpu.make_async_remote_copy(
            src_ref=part_out,
            dst_ref=part_in,
            send_sem=core_send.at[0],
            recv_sem=core_recv.at[0],
            device_id={"date": d + 1 - 2 * core},
            device_id_type=MESH,
        )

    def to_relay(side):
        half = pl.ds(2 * side, 2)
        return pltpu.make_async_remote_copy(
            src_ref=own.at[0, half],
            dst_ref=relay_in.at[side],
            send_sem=relay_send.at[side],
            recv_sem=relay_recv.at[side],
            device_id={"date": 2 * lax.rem(z + (1 if side == 0 else rings - 1), rings) + core},
            device_id_type=MESH,
        )

    def to_all(buffer, axis, me, size, send, recv, k):
        return pltpu.make_async_remote_copy(
            src_ref=buffer.at[me],
            dst_ref=buffer.at[me],
            send_sem=send.at[0],
            recv_sem=recv.at[0],
            device_id={axis: lax.rem(me + k, size)},
            device_id_type=MESH,
        )

    def whole_of(buffer, axis, me, size, send, recv):
        others = buffer.at[pl.ds(0, size - 1)]
        return pltpu.make_async_remote_copy(
            src_ref=others,
            dst_ref=others,
            send_sem=send.at[0],
            recv_sem=recv.at[0],
            device_id={axis: lax.rem(me + 1, size)},
            device_id_type=MESH,
        )

    to_pix = (pix_in, "pix", p, pixs, pix_send, pix_recv)
    to_date = (date_in, "date", d, dates, date_send, date_recv)
    to_level = (level_in, "date", d, dates, level_send, level_recv)

    def body(acc_a, acc_b, acc_c, acc_d, acc_prefix, acc_rows, acc_sums, acc_ta, acc_tb):
        tile_acc[...] = jnp.zeros_like(tile_acc)

        accs = (acc_a, acc_b, acc_c, acc_d)

        def step(s, carry):
            codes, last = carry
            ahead, half_a, half_b = lax.rem(codes[0], rings), lax.rem(codes[1], 2), lax.rem(codes[2], 2)
            behind = lax.rem(rings - ahead, rings)

            @pl.when((s == 0) | (half_a == 0))
            def _():
                for copy in load(ahead):
                    copy.wait()

            @pl.when((s > 0) & (s < rings - 1) & (half_a == 0))
            def _():
                for copy in load(behind):
                    copy.wait()

            ring_a, ring_b = lax.rem(z + ahead, rings), lax.rem(z + behind, rings)

            def base_of(m):
                side = 1 - core if m < 4 else core
                ring, half = (ring_a, half_a) if m % 4 < 2 else (ring_b, half_b)
                return (2 * ring + side) * owner_lanes + (2 * half + m % 2) * (JOINED * BLOCK)

            sums = None
            for m in range(8):
                feed_group(idx_v, w_v, base_of(m), accs[m % 4], m % 2)
                if m < 6:
                    counts = drain_group(accs[m % 4])
                    if m < 4:
                        part_out[s, m] = counts
                    else:
                        raw[s, m - 4] = counts
                    sums = counts if sums is None else sums + counts
            tile_acc[...] += sums

            @pl.when(s == 0)
            def _():
                pl.semaphore_wait(barrier, dates + pixs - 2)

            to_core(s).start()

            @pl.when(s >= 1)
            def _():
                to_core(s - 1).wait_recv()
                own[s - 1] = raw[s - 1] + part_in[s - 1]

            @pl.when(s == 1)
            def _():
                to_relay(0).start()
                to_relay(1).start()

            for side in range(2):
                at = FIRST_RELAYED + side

                @pl.when(s == at + 1)
                def _(side=side, at=at):
                    to_relay(side).wait_recv()
                    own[at, 2 * side : 2 * side + 2] += relay_in[side]

            @pl.when(s >= 2)
            def _():
                to_ring(s - 1, last[0], 0, last[1]).start()
                to_ring(s - 1, rings - last[0], 1, last[1]).start()

            for m in (6, 7):
                counts = drain_group(accs[m % 4])
                raw[s, m - 4] = counts
                tile_acc[...] += counts
            return (lax.div(codes[0], rings), lax.div(codes[1], 2), lax.div(codes[2], 2)), (ahead, half_a)

        codes = (
            jnp.int32(sum(v * rings**s for s, v in enumerate(AHEAD))),
            jnp.int32(sum(v * 2**s for s, v in enumerate(HALF_AHEAD))),
            jnp.int32(sum(v * 2**s for s, v in enumerate(HALF_BEHIND))),
        )
        lax.fori_loop(0, rings, step, (codes, (jnp.int32(0), jnp.int32(0))))

        lane = iota((8, 128), 1)
        folded = tile_acc[:, :128] + tile_acc[:, 128:]
        folded = folded + pltpu.roll(folded, 64, 1)
        pix_in[p] = jnp.where(lane < 64, folded[:8], folded[8:])
        for k in range(1, pixs):
            to_all(*to_pix, k).start()
        push_tile_tables(1)

        to_core(rings - 1).wait_recv()
        mine = raw[rings - 1] + part_in[rings - 1]

        all_rings().wait_recv()
        for off in range(1, rings):
            if off != rings // 2:
                mine = mine + ici_in[off]
        level_in[d] = block_levels(mine, acc_prefix, acc_rows, acc_a, acc_sums)
        for k in range(1, dates):
            to_all(*to_level, k).start()

        whole_of(*to_pix).wait_recv()
        total = pix_in[0]
        for k in range(1, pixs):
            total = total + pix_in[k]
        date_in[d] = total
        for k in range(1, dates):
            to_all(*to_date, k).start()

        all_cores().wait_send()
        for side in range(2):
            to_relay(side).wait_send()
        all_rings().wait_send()
        whole_of(*to_pix).wait_send()

        whole_of(*to_date).wait_recv()
        total = date_in[0]
        for k in range(1, dates):
            total = total + date_in[k]
        levels = tile_of(total, acc_ta, acc_tb, 1)
        row = iota((8, 128), 0)
        by_lane = jnp.where(lane == 0, levels[0], jnp.where(lane == 1, levels[1], levels[2]))
        by_row = jnp.where(row == 0, levels[0], jnp.where(row == 1, levels[1], levels[2]))
        tile_ref[...] = by_lane[:1]

        whole_of(*to_level).wait_recv()
        for v in range(4):
            wide = level_in[4 * v]
            for i in range(1, 4):
                wide = jnp.where(lane >= 32 * i, level_in[4 * v + i], wide)
            anomaly_ref[:, v * 128 : (v + 1) * 128] = (wide - by_row)[:3]

        whole_of(*to_date).wait_send()
        whole_of(*to_level).wait_send()

    pl.run_scoped(
        body,
        pltpu.ACC(0)((128, 256), f32),
        pltpu.ACC(1)((128, 256), f32),
        pltpu.ACC(0)((128, 256), f32),
        pltpu.ACC(1)((128, 256), f32),
        pltpu.ACC(0)((64, 256), f32),
        pltpu.ACC(1)((64, 256), f32),
        pltpu.ACC(1)((48, 256), f32),
        pltpu.ACC(0)((16, 256), f32),
        pltpu.ACC(1)((16, 256), f32),
    )


def finish(anomaly_ref, tile_ref, anomaly_out, tile_out):
    anomaly_out[...] = anomaly_ref[...]
    tile_out[...] = tile_ref[0, :3]


def solution(mesh):
    dates, pixs = mesh.shape["date"], mesh.shape["pix"]
    rings = dates // 2
    assert rings == len(AHEAD)

    def body(bin_index, clear_mask):
        frames, pixels = bin_index.shape
        blocks = pixels // BLOCK
        groups = blocks // dates // JOINED
        quarter = (rings, groups, UPPER, JOINED * LOWER)
        dma = pltpu.SemaphoreType.DMA
        anomaly, tile = pl.pallas_call(
            functools.partial(kernel, dates, pixs),
            out_shape=(
                jax.ShapeDtypeStruct((3, blocks), f32),
                jax.ShapeDtypeStruct((1, 128), f32),
            ),
            in_specs=[pl.BlockSpec(memory_space=pltpu.HBM)] * 2,
            out_specs=(pl.BlockSpec(memory_space=pltpu.VMEM),) * 2,
            scratch_shapes=[
                pltpu.VMEM((frames, pixels), jnp.int32),
                pltpu.VMEM((frames, pixels), bf16),
                *[pltpu.VMEM(quarter, f32) for _ in range(5)],
                pltpu.VMEM((2, 2, UPPER, JOINED * LOWER), f32),
                pltpu.VMEM((UPPER, JOINED * LOWER), f32),
                pltpu.VMEM((pixs, 8, 128), f32),
                pltpu.VMEM((dates, 8, 128), f32),
                pltpu.VMEM((dates, 8, 128), f32),
                dma((2, rings)),
                dma((1,)),
                dma((rings,)),
                dma((1,)),
                dma((1,)),
                dma((2,)),
                dma((2,)),
                *[dma((1,)) for _ in range(6)],
            ],
            compiler_params=pltpu.CompilerParams(
                collective_id=0, has_side_effects=True, vmem_limit_bytes=52 * 1024 * 1024
            ),
        )(bin_index, clear_mask)
        return pl.pallas_call(
            finish,
            out_shape=(
                jax.ShapeDtypeStruct((3, blocks), f32),
                jax.ShapeDtypeStruct((3,), f32),
            ),
            in_specs=[pl.BlockSpec(memory_space=pltpu.VMEM)] * 2,
            out_specs=(pl.BlockSpec(memory_space=pltpu.VMEM),) * 2,
            compiler_params=pltpu.CompilerParams(vmem_limit_bytes=1024 * 1024),
        )(anomaly, tile)

    return jax.shard_map(
        body,
        mesh=mesh,
        in_specs=(P("date", "pix"), P("date", "pix")),
        out_specs=(P(None, "pix"), P()),
        check_vma=False,
    )
```

```python
import functools

import jax
import jax.numpy as jnp
from jax import lax
from jax.experimental import pallas as pl
from jax.experimental.pallas import tpu as pltpu
from jax.sharding import PartitionSpec as P

BINS = 512
BLOCK = 128
UPPER = 16
LOWER = 32
JOINED = 8
QUANTILES = (0.1, 0.5, 0.9)
LOW_EDGE = -1.0
AHEAD = (4, 2, 2, 3, 3, 1, 1, 0)
HALF_AHEAD = (0, 0, 1, 0, 1, 0, 1, 0)
HALF_BEHIND = (1, 0, 1, 0, 1, 0, 1, 1)
FIRST_RELAYED = 3
MESH = pl.DeviceIdType.MESH
bf16 = jnp.bfloat16
f32 = jnp.float32
f8 = jnp.float8_e4m3fn


def iota(shape, dim):
    return lax.broadcasted_iota(jnp.int32, shape, dim)


def ones_where(mask):
    return jnp.where(mask, 1.0, 0.0).astype(bf16)


def pieces(x):
    first = x.astype(bf16)
    rest = x - first.astype(f32)
    second = rest.astype(bf16)
    third = (rest - second.astype(f32)).astype(bf16)
    return first, second, third


def feed_group(idx_ref, w_ref, base, acc, mxu):
    upper_rows = (iota((UPPER, 128), 0) * LOWER).astype(jnp.int16)
    lower_rows = iota((LOWER, 128), 0).astype(jnp.int16)
    lefts, rights = [], []
    frames = idx_ref.shape[0]
    for j in range(JOINED):
        lanes = pl.ds(pl.multiple_of(base + 128 * j, 128), 128)
        bins = idx_ref[:, lanes].astype(jnp.int16)
        weight = w_ref[:, lanes]
        upper = bins & jnp.int16((UPPER - 1) * LOWER)
        lower = bins & jnp.int16(LOWER - 1)
        left, right = [], []
        for f in range(frames):
            row = slice(f, f + 1)
            is_upper = jnp.broadcast_to(upper[row], (UPPER, 128)) == upper_rows
            is_lower = jnp.broadcast_to(lower[row], (LOWER, 128)) == lower_rows
            left.append(jnp.where(is_upper, jnp.broadcast_to(weight[row], (UPPER, 128)), jnp.zeros((), bf16)))
            right.append(jnp.where(is_lower, jnp.ones((), f8), jnp.zeros((), f8)))
        lefts.append(left)
        rights.append(right)
    for k in range(frames // 2):
        pair = (2 * k, 2 * k + 1)
        left = jnp.concatenate([jnp.concatenate([x[f] for f in pair], axis=1) for x in lefts], axis=0)
        right = jnp.concatenate([jnp.concatenate([x[f] for f in pair], axis=1) for x in rights], axis=0)
        pltpu.matmul_push_rhs(right, staging_register=k % 2, mxu_index=mxu, transpose=True)
        pltpu.matmul_acc_lhs(acc, left, load_staged_rhs=k % 2)


def drain_group(acc):
    joint = pltpu.matmul_pop(acc)
    lane = iota((UPPER, 128), 1)
    halves = []
    for half in range(2):
        own = None
        for q in range(4):
            j = 4 * half + q
            part = joint[j * UPPER : (j + 1) * UPPER, half * 128 : (half + 1) * 128]
            own = part if own is None else jnp.where(lane >= q * LOWER, part, own)
        halves.append(own)
    return jnp.concatenate(halves, axis=1)


def triple_matmul(acc, x, register):
    for n, piece in enumerate(pieces(x)):
        pltpu.matmul_acc_lhs(acc, piece, load_staged_rhs=register if n == 0 else None)


def build_level_tables(chosen_ref, sums_ref):
    r, c = iota((256, 256), 0), iota((256, 256), 1)
    same = (r // LOWER) == (c // LOWER)
    pltpu.matmul_push_rhs(ones_where(same & (r % LOWER < c % LOWER)), staging_register=0, mxu_index=0)
    pltpu.matmul_push_rhs(ones_where(same), staging_register=0, mxu_index=1)
    i, k = iota((128, 256), 0), iota((128, 256), 1)
    chosen_ref[...] = ones_where(
        ((i % 64) // UPPER == (k % 64) // UPPER) & (k < 192) & ((k % UPPER < i % UPPER) | (i >= 64))
    )
    for g in range(4):
        sums_ref[g] = ones_where((c % LOWER) == JOINED * g + r // LOWER)


def block_levels(counts, chosen_ref, sums_ref, acc_prefix, acc_rows, acc_below, acc_sums):
    flat = counts.reshape(64, 256)
    triple_matmul(acc_rows, flat, 0)
    triple_matmul(acc_prefix, flat, 0)
    row_sums = pltpu.matmul_pop(acc_rows)
    stacked = jnp.concatenate([*pieces(row_sums), jnp.zeros((64, 256), bf16)], axis=0)
    pltpu.matmul_push_rhs(stacked, staging_register=0, mxu_index=0)
    pltpu.matmul_acc_lhs(acc_below, chosen_ref[...], load_staged_rhs=0)
    within = pltpu.matmul_pop(acc_prefix)
    below = pltpu.matmul_pop(acc_below)
    before = within + below[:64]
    total = below[64:]
    floor = jnp.maximum(flat, 1.0)
    passed = [jnp.clip((q * total + 0.25 - before) / floor, 0.0, 1.0) for q in QUANTILES]
    for g in range(4):
        pltpu.matmul_push_rhs(sums_ref[g], staging_register=0, mxu_index=1)
        rows = jnp.concatenate([p[g * UPPER : (g + 1) * UPPER] for p in passed], axis=0)
        triple_matmul(acc_sums, rows, 0)
    sums = pltpu.matmul_pop(acc_sums)[:, :128]
    row = iota((4, 128), 0)
    out = jnp.zeros((4, 128), f32)
    for q in range(3):
        value = jnp.sum(sums[q * UPPER : (q + 1) * UPPER], axis=0, keepdims=True)
        out = jnp.where(row == q, LOW_EDGE + 2.0 / BINS * value, out)
    return out


def push_tile_tables(register):
    r, c = iota((256, 256), 0), iota((256, 256), 1)
    r_part, c_part = (r % 128) // LOWER, (c % 128) // LOWER
    same = r_part == c_part
    prefix = same & (r % LOWER < c % LOWER)
    pltpu.matmul_push_rhs(ones_where((c >= 128) | prefix), staging_register=register, mxu_index=0)
    pltpu.matmul_push_rhs(
        ones_where(((c < 128) & same) | ((c >= 128) & (r_part < c_part))), staging_register=register, mxu_index=1
    )


def tile_of(total, acc_a, acc_b, register):
    counts = jnp.concatenate([total, jnp.zeros((4, 128), f32)], axis=0)
    p1, p2, p3 = pieces(counts)
    zero = jnp.zeros((8, 128), f32)
    left = jnp.concatenate(
        [
            jnp.concatenate([p1.astype(f32), p3.astype(f32)], axis=0),
            jnp.concatenate([p2.astype(f32), zero], axis=0),
        ],
        axis=1,
    ).astype(bf16)
    pltpu.matmul_acc_lhs(acc_a, left, load_staged_rhs=register)
    pltpu.matmul_acc_lhs(acc_b, left, load_staged_rhs=register)
    a = pltpu.matmul_pop(acc_a)
    b = pltpu.matmul_pop(acc_b)
    a = a[:8] + a[8:]
    b = b[:8] + b[8:]
    within, all_rows = a[:, :128], a[:, 128:]
    same_rows, parts_below = b[:, :128], b[:, 128:]
    row = iota((8, 128), 0)
    below = jnp.where(row >= 1, pltpu.roll(same_rows, 1, 0), 0.0)
    for shift in (1, 2):
        below = below + jnp.where(row >= shift, pltpu.roll(below, shift, 0), 0.0)
    for shift in (1, 2, 4):
        all_rows = all_rows + pltpu.roll(all_rows, shift, 0)
        parts_below = parts_below + pltpu.roll(parts_below, shift, 0)
    before = within + below + parts_below
    floor = jnp.maximum(counts, 1.0)
    levels = []
    for q in QUANTILES:
        passed = jnp.clip((q * all_rows + 0.25 - before) / floor, 0.0, 1.0)
        passed = jnp.where(row < 4, passed, 0.0)
        passed = jnp.sum(jnp.sum(passed, axis=0, keepdims=True), axis=1, keepdims=True)
        levels.append(LOW_EDGE + 2.0 / BINS * passed)
    return levels


def kernel(
    dates,
    pixs,
    idx_hbm,
    w_hbm,
    anomaly_ref,
    tile_ref,
    idx_v,
    w_v,
    raw,
    part_out,
    part_in,
    own,
    ici_in,
    relay_in,
    tile_acc,
    chosen_ref,
    sums_ref,
    pix_in,
    date_in,
    level_in,
    in_sem,
    core_send,
    core_recv,
    ici_send,
    ici_recv,
    relay_send,
    relay_recv,
    pix_send,
    pix_recv,
    date_send,
    date_recv,
    level_send,
    level_recv,
):
    d = lax.axis_index("date")
    p = lax.axis_index("pix")
    z = lax.div(d, 2)
    core = lax.rem(d, 2)
    rings = dates // 2
    owner_lanes = idx_v.shape[1] // dates
    chunk = 2 * owner_lanes

    def load(off):
        ring = lax.rem(z + off, rings)
        lanes = pl.ds(pl.multiple_of(ring * chunk, 128), chunk)
        return (
            pltpu.make_async_copy(idx_hbm.at[:, lanes], idx_v.at[:, lanes], in_sem.at[0, ring]),
            pltpu.make_async_copy(w_hbm.at[:, lanes], w_v.at[:, lanes], in_sem.at[1, ring]),
        )

    for copy in load(AHEAD[0]):
        copy.start()
    barrier = pltpu.get_barrier_semaphore()
    for k in range(1, dates):
        pl.semaphore_signal(barrier, inc=1, device_id={"date": lax.rem(d + k, dates)}, device_id_type=MESH)
    for k in range(1, pixs):
        pl.semaphore_signal(barrier, inc=1, device_id={"pix": lax.rem(p + k, pixs)}, device_id_type=MESH)

    for off in (2, 6, 3, 5, 1, 7, 0):
        for copy in load(off):
            copy.start()

    def to_core(s):
        return pltpu.make_async_remote_copy(
            src_ref=part_out.at[s],
            dst_ref=part_in.at[s],
            send_sem=core_send.at[0],
            recv_sem=core_recv.at[s],
            device_id={"date": d + 1 - 2 * core},
            device_id_type=MESH,
        )

    def to_ring(s, off, side, half):
        groups = pl.ds(2 * half, 2)
        return pltpu.make_async_remote_copy(
            src_ref=own.at[s, pl.ds(2 * side, 2)],
            dst_ref=ici_in.at[off, groups],
            send_sem=ici_send.at[0],
            recv_sem=ici_recv.at[0],
            device_id={"date": 2 * lax.rem(z + off, rings) + core},
            device_id_type=MESH,
        )

    def all_rings():
        whole = own.at[pl.ds(0, rings - 2)]
        return pltpu.make_async_remote_copy(
            src_ref=whole,
            dst_ref=ici_in.at[pl.ds(0, rings - 2)],
            send_sem=ici_send.at[0],
            recv_sem=ici_recv.at[0],
            device_id={"date": d + 1 - 2 * core},
            device_id_type=MESH,
        )

    def all_cores():
        return pltpu.make_async_remote_copy(
            src_ref=part_out,
            dst_ref=part_in,
            send_sem=core_send.at[0],
            recv_sem=core_recv.at[0],
            device_id={"date": d + 1 - 2 * core},
            device_id_type=MESH,
        )

    def to_relay(side):
        half = pl.ds(2 * side, 2)
        return pltpu.make_async_remote_copy(
            src_ref=own.at[0, half],
            dst_ref=relay_in.at[side],
            send_sem=relay_send.at[side],
            recv_sem=relay_recv.at[side],
            device_id={"date": 2 * lax.rem(z + (1 if side == 0 else rings - 1), rings) + core},
            device_id_type=MESH,
        )

    def to_all(buffer, axis, me, size, send, recv, k):
        return pltpu.make_async_remote_copy(
            src_ref=buffer.at[me],
            dst_ref=buffer.at[me],
            send_sem=send.at[0],
            recv_sem=recv.at[0],
            device_id={axis: lax.rem(me + k, size)},
            device_id_type=MESH,
        )

    def whole_of(buffer, axis, me, size, send, recv):
        others = buffer.at[pl.ds(0, size - 1)]
        return pltpu.make_async_remote_copy(
            src_ref=others,
            dst_ref=others,
            send_sem=send.at[0],
            recv_sem=recv.at[0],
            device_id={axis: lax.rem(me + 1, size)},
            device_id_type=MESH,
        )

    to_pix = (pix_in, "pix", p, pixs, pix_send, pix_recv)
    to_date = (date_in, "date", d, dates, date_send, date_recv)
    to_level = (level_in, "date", d, dates, level_send, level_recv)

    def body(acc_a, acc_b, acc_c, acc_d, acc_prefix, acc_rows, acc_sums, acc_ta, acc_tb):
        tile_acc[...] = jnp.zeros_like(tile_acc)

        accs = (acc_a, acc_b, acc_c, acc_d)

        def step(s, carry):
            codes, last = carry
            ahead, half_a, half_b = lax.rem(codes[0], rings), lax.rem(codes[1], 2), lax.rem(codes[2], 2)
            behind = lax.rem(rings - ahead, rings)

            @pl.when((s == 0) | (half_a == 0))
            def _():
                for copy in load(ahead):
                    copy.wait()

            @pl.when((s > 0) & (s < rings - 1) & (half_a == 0))
            def _():
                for copy in load(behind):
                    copy.wait()

            ring_a, ring_b = lax.rem(z + ahead, rings), lax.rem(z + behind, rings)

            def base_of(m):
                side = 1 - core if m < 4 else core
                ring, half = (ring_a, half_a) if m % 4 < 2 else (ring_b, half_b)
                return (2 * ring + side) * owner_lanes + (2 * half + m % 2) * (JOINED * BLOCK)

            sums = None
            for m in range(8):
                feed_group(idx_v, w_v, base_of(m), accs[m % 4], m % 2)
                if m < 6:
                    counts = drain_group(accs[m % 4])
                    if m < 4:
                        part_out[s, m] = counts
                    else:
                        raw[s, m - 4] = counts
                    sums = counts if sums is None else sums + counts
            tile_acc[...] += sums

            @pl.when(s == 0)
            def _():
                pl.semaphore_wait(barrier, dates + pixs - 2)

            to_core(s).start()

            @pl.when(s >= 1)
            def _():
                to_core(s - 1).wait_recv()
                own[s - 1] = raw[s - 1] + part_in[s - 1]

            @pl.when(s == 1)
            def _():
                to_relay(0).start()
                to_relay(1).start()

            for side in range(2):
                at = FIRST_RELAYED + side

                @pl.when(s == at + 1)
                def _(side=side, at=at):
                    to_relay(side).wait_recv()
                    own[at, 2 * side : 2 * side + 2] += relay_in[side]

            @pl.when(s >= 2)
            def _():
                to_ring(s - 1, last[0], 0, last[1]).start()
                to_ring(s - 1, rings - last[0], 1, last[1]).start()

            for m in (6, 7):
                counts = drain_group(accs[m % 4])
                raw[s, m - 4] = counts
                tile_acc[...] += counts
            return (lax.div(codes[0], rings), lax.div(codes[1], 2), lax.div(codes[2], 2)), (ahead, half_a)

        codes = (
            jnp.int32(sum(v * rings**s for s, v in enumerate(AHEAD))),
            jnp.int32(sum(v * 2**s for s, v in enumerate(HALF_AHEAD))),
            jnp.int32(sum(v * 2**s for s, v in enumerate(HALF_BEHIND))),
        )
        lax.fori_loop(0, rings, step, (codes, (jnp.int32(0), jnp.int32(0))))

        folded = tile_acc[:, :128] + tile_acc[:, 128:]
        folded = folded + pltpu.roll(folded, 64, 1)
        folded = folded + pltpu.roll(folded, 32, 1)
        lane = iota((4, 128), 1)
        packed = folded[:4]
        for i in range(1, 4):
            packed = jnp.where(lane >= 32 * i, folded[4 * i : 4 * i + 4], packed)
        pix_in[p] = packed
        for k in range(1, pixs):
            to_all(*to_pix, k).start()
        push_tile_tables(1)
        build_level_tables(chosen_ref, sums_ref)

        to_core(rings - 1).wait_recv()
        raw[rings - 1] += part_in[rings - 1]

        whole_of(*to_pix).wait_recv()
        total = pix_in[0]
        for k in range(1, pixs):
            total = total + pix_in[k]
        date_in[d] = total
        for k in range(1, dates):
            to_all(*to_date, k).start()

        all_rings().wait_recv()
        mine = raw[rings - 1]
        for off in range(1, rings):
            if off != rings // 2:
                mine = mine + ici_in[off]
        level_in[d] = block_levels(mine, chosen_ref, sums_ref, acc_prefix, acc_rows, acc_a, acc_sums)
        for k in range(1, dates):
            to_all(*to_level, k).start()

        all_cores().wait_send()
        for side in range(2):
            to_relay(side).wait_send()
        all_rings().wait_send()
        whole_of(*to_pix).wait_send()

        whole_of(*to_date).wait_recv()
        total = date_in[0]
        for k in range(1, dates):
            total = total + date_in[k]
        levels = tile_of(total, acc_ta, acc_tb, 1)
        row = iota((4, 128), 0)
        by_lane = jnp.where(lane == 0, levels[0], jnp.where(lane == 1, levels[1], levels[2]))
        by_row = jnp.where(row == 0, levels[0], jnp.where(row == 1, levels[1], levels[2]))
        tile_ref[...] = by_lane[:1]

        whole_of(*to_level).wait_recv()
        for v in range(4):
            wide = level_in[4 * v]
            for i in range(1, 4):
                wide = jnp.where(lane >= 32 * i, level_in[4 * v + i], wide)
            anomaly_ref[:, v * 128 : (v + 1) * 128] = (wide - by_row)[:3]

        whole_of(*to_date).wait_send()
        whole_of(*to_level).wait_send()

    pl.run_scoped(
        body,
        pltpu.ACC(0)((128, 256), f32),
        pltpu.ACC(1)((128, 256), f32),
        pltpu.ACC(0)((128, 256), f32),
        pltpu.ACC(1)((128, 256), f32),
        pltpu.ACC(0)((64, 256), f32),
        pltpu.ACC(1)((64, 256), f32),
        pltpu.ACC(1)((48, 256), f32),
        pltpu.ACC(0)((16, 256), f32),
        pltpu.ACC(1)((16, 256), f32),
    )


def finish(anomaly_ref, tile_ref, anomaly_out, tile_out):
    anomaly_out[...] = anomaly_ref[...]
    tile_out[...] = tile_ref[0, :3]


def solution(mesh):
    dates, pixs = mesh.shape["date"], mesh.shape["pix"]
    rings = dates // 2
    assert rings == len(AHEAD)

    def body(bin_index, clear_mask):
        frames, pixels = bin_index.shape
        blocks = pixels // BLOCK
        groups = blocks // dates // JOINED
        quarter = (rings, groups, UPPER, JOINED * LOWER)
        dma = pltpu.SemaphoreType.DMA
        anomaly, tile = pl.pallas_call(
            functools.partial(kernel, dates, pixs),
            out_shape=(
                jax.ShapeDtypeStruct((3, blocks), f32),
                jax.ShapeDtypeStruct((1, 128), f32),
            ),
            in_specs=[pl.BlockSpec(memory_space=pltpu.HBM)] * 2,
            out_specs=(pl.BlockSpec(memory_space=pltpu.VMEM),) * 2,
            scratch_shapes=[
                pltpu.VMEM((frames, pixels), jnp.int32),
                pltpu.VMEM((frames, pixels), bf16),
                *[pltpu.VMEM(quarter, f32) for _ in range(5)],
                pltpu.VMEM((2, 2, UPPER, JOINED * LOWER), f32),
                pltpu.VMEM((UPPER, JOINED * LOWER), f32),
                pltpu.VMEM((128, 256), bf16),
                pltpu.VMEM((4, 256, 256), bf16),
                pltpu.VMEM((pixs, 4, 128), f32),
                pltpu.VMEM((dates, 4, 128), f32),
                pltpu.VMEM((dates, 4, 128), f32),
                dma((2, rings)),
                dma((1,)),
                dma((rings,)),
                dma((1,)),
                dma((1,)),
                dma((2,)),
                dma((2,)),
                *[dma((1,)) for _ in range(6)],
            ],
            compiler_params=pltpu.CompilerParams(
                collective_id=0, has_side_effects=True, vmem_limit_bytes=52 * 1024 * 1024
            ),
        )(bin_index, clear_mask)
        return pl.pallas_call(
            finish,
            out_shape=(
                jax.ShapeDtypeStruct((3, blocks), f32),
                jax.ShapeDtypeStruct((3,), f32),
            ),
            in_specs=[pl.BlockSpec(memory_space=pltpu.VMEM)] * 2,
            out_specs=(pl.BlockSpec(memory_space=pltpu.VMEM),) * 2,
            compiler_params=pltpu.CompilerParams(vmem_limit_bytes=1024 * 1024),
        )(anomaly, tile)

    return jax.shard_map(
        body,
        mesh=mesh,
        in_specs=(P("date", "pix"), P("date", "pix")),
        out_specs=(P(None, "pix"), P()),
        check_vma=False,
    )
```
